32 devices in a mesh: ctx: 16 (over z, y, x), head: 2 (over core).
Axes of the slice: x: 2, y: 2, z: 4, core: 2. Of those that a mesh axis runs over, the one named last changes fastest.
Arguments:
- query: bfloat16 [2048, 384], P('ctx', 'head'), may hold values from -48 to 48
- key_nope: bfloat16 [2048, 256], P('ctx', 'head'), may hold values from -8 to 8
- key_rope: bfloat16 [2048, 64], P('ctx'), may hold values from -8 to 8
- value: bfloat16 [2048, 256], P('ctx', 'head'), may hold values from -6 to 6
- d_out: bfloat16 [2048, 256], P('ctx', 'head'), may hold values from -288 to 288
- positions: int32 [2048], P('ctx'), may hold values from 0 to 2047, as said below
- segments: int32 [2048], replicated, may hold values from 0 to 3, never falling along the last dimension, each value on 1 to 1024 neighbouring positions
Outputs:
- d_query: bfloat16 [2048, 384], P('ctx', 'head')
- d_key_nope: bfloat16 [2048, 256], P('ctx', 'head')
- d_key_rope: bfloat16 [2048, 64], P('ctx')
- d_value: bfloat16 [2048, 256], P('ctx', 'head')
The draws below stay inside these ranges and needn't reach their ends.
Inputs may be any that keep to these rules, and one draw needn't show every extreme that they name: A permutation of 0 to 2047 made of aligned blocks of 32 rows holding 32 consecutive positions in order.
All inputs are finite; a program needn't handle non-finite values.
Results may differ from the reference program's by a relative error of at most 0.0049.
Values may be sent and summed in bfloat16 or wider, within the bound.
A program may use at most 64 MiB of HBM per device.

```python
import math
import jax
import jax.numpy as jnp
import numpy as np
from jax import lax

NOPE = 128
ROPE = 64
VD = 128
BLK = 32
DOCS = 4
QK = 192
HEADS = 2
TOKENS = 2048


def block_positions(key):
    block_total = TOKENS // BLK
    order = jax.random.permutation(jax.random.fold_in(key, 101), block_total).astype(jnp.int32)
    within = jnp.arange(BLK, dtype=jnp.int32)
    return (order[:, None] * BLK + within[None, :]).reshape(TOKENS)


def draw_positions(key, part):
    return block_positions(key)


def attention_operands(key):
    base_query = jnp.clip(jax.random.normal(jax.random.fold_in(key, 201), (TOKENS, HEADS, QK), jnp.float32), -6.0, 6.0)
    base_nope = jnp.clip(jax.random.normal(jax.random.fold_in(key, 202), (TOKENS, HEADS, NOPE), jnp.float32), -6.0, 6.0)
    base_rope = jnp.clip(jax.random.normal(jax.random.fold_in(key, 203), (TOKENS, ROPE), jnp.float32), -6.0, 6.0)
    return (base_query, base_nope, base_rope)


def draw_query(key, part):
    base_query, base_nope, base_rope = attention_operands(key)
    return base_query.reshape(TOKENS, HEADS * QK).astype(jnp.bfloat16)


def draw_key_nope(key, part):
    base_query, base_nope, base_rope = attention_operands(key)
    return base_nope.reshape(TOKENS, HEADS * NOPE).astype(jnp.bfloat16)


def draw_key_rope(key, part):
    base_query, base_nope, base_rope = attention_operands(key)
    return base_rope.astype(jnp.bfloat16)


def draw_d_out(key, part):
    ramp = jnp.arange(TOKENS, dtype=jnp.int32).astype(jnp.float32) / TOKENS
    rising = jnp.exp(math.log(3.0) * ramp)
    base = jnp.clip(jax.random.normal(jax.random.fold_in(key, 301), (TOKENS, HEADS * VD), jnp.float32), -6.0, 6.0)
    magnitude = 16.0
    return (magnitude * base * rising[:, None]).astype(jnp.bfloat16)


def level_of(stream_key, dims, pieces, smallest, high):
    factor_of = 1.0
    for axis_at, blocks in pieces:
        draws = jax.random.uniform(jax.random.fold_in(jax.random.fold_in(stream_key, 6), axis_at), (blocks,), jnp.float32, smallest / len(pieces), high / len(pieces))
        factor_of = factor_of * jnp.repeat(jnp.exp(draws), dims[axis_at] // blocks).reshape((-1,) + (1,) * (len(dims) - 1 - axis_at))
    return factor_of


def split_up(count, total, bound, skew):
    weights = [(1 << 20) // math.isqrt(rank ** skew) + 1 for rank in range(2, count + 1)]
    spare, holding = total - bound - (count - 1), [1] * (count - 1)
    while spare > 0:
        movable = [i for i in range(count - 1) if holding[i] < bound]
        mass, remaining = sum([weights[i] for i in movable]), spare
        for i in movable:
            addition = min(bound - holding[i], max(1, remaining * weights[i] // mass), spare)
            holding[i] = holding[i] + addition
            spare = spare - addition
    return np.array([bound] + holding)


def uneven(key, number_of, total, most, slope):
    if number_of == 2:
        one = jax.random.randint(key, (), max(1, total - most), min(most, total - 1) + 1)
        return jnp.stack([one, total - one])
    lengths = jnp.asarray(split_up(number_of, total, most, slope), jnp.int32)
    couples = (number_of - 1) // 2
    donor, sink = lengths[1:1 + 2 * couples:2], lengths[2:2 + 2 * couples:2]
    margin = jnp.minimum(donor - 1, most - sink)
    passed = jax.random.randint(jax.random.fold_in(key, 1), (couples,), 0, 1 << 20) % (margin + 1)
    lengths = lengths.at[1:1 + 2 * couples:2].set(donor - passed).at[2:2 + 2 * couples:2].set(sink + passed)
    return lengths[jax.random.permutation(jax.random.fold_in(key, 2), number_of)]


def centred(rng, extent, spread, bound, pieces=(), held_as=jnp.bfloat16):
    entries = spread * jax.random.normal(rng, extent, jnp.float32)
    if pieces:
        entries = entries * level_of(rng, extent, pieces, -0.22, 0.18)
    return jnp.clip(entries, -bound, bound).astype(held_as)


def setup_inputs(seed: int = 0) -> dict:
    splits = jax.random.split(jax.random.key(seed), 8)
    query = draw_query(jax.random.fold_in(splits[7], 71), 0)
    key_nope = draw_key_nope(jax.random.fold_in(splits[7], 71), 0)
    key_rope = draw_key_rope(jax.random.fold_in(splits[7], 71), 0)
    value = centred(splits[3], (TOKENS, HEADS * VD), 1.0, 6.0, ((0, 16), (1, 2)))
    d_out = draw_d_out(jax.random.fold_in(splits[7], 71), 0)
    positions = draw_positions(jax.random.fold_in(splits[7], 71), 0)
    segments = jnp.searchsorted(jnp.cumsum(uneven(splits[6], DOCS, TOKENS, TOKENS // 2, 2)), jnp.arange(TOKENS), side="right").astype(jnp.int32)
    return {"query": query, "key_nope": key_nope, "key_rope": key_rope, "value": value, "d_out": d_out, "positions": positions, "segments": segments}


def head_grads(operands, key_rope, positions, documents):
    query_head, nope_head, value_head, dout_head = operands
    softmax_scale = 1.0 / math.sqrt(QK)
    key_rows = jnp.concatenate([nope_head, key_rope], axis=1)
    block_rows = math.gcd(TOKENS, 1024)
    block_count = TOKENS // block_rows

    def visit(carried, block_index):
        grad_key, grad_value = carried
        offset = (block_index * block_rows).astype(jnp.int32)
        query_block = lax.dynamic_slice_in_dim(query_head, offset, block_rows, 0)
        dout_block = lax.dynamic_slice_in_dim(dout_head, offset, block_rows, 0)
        place_block = lax.dynamic_slice_in_dim(positions, offset, block_rows, 0)
        doc_block = lax.dynamic_slice_in_dim(documents, offset, block_rows, 0)
        scores = jnp.dot(query_block, key_rows.T, preferred_element_type=jnp.float32) * softmax_scale
        visible_pairs = (doc_block[:, None] == documents[None, :]) & (positions[None, :] <= place_block[:, None])
        scores = jnp.where(visible_pairs, scores, -jnp.inf)
        row_max = lax.optimization_barrier(jnp.max(scores, axis=1, keepdims=True))
        log_total = row_max + jnp.log(lax.optimization_barrier(jnp.sum(jnp.exp(scores - row_max), axis=1, keepdims=True)))
        weights = jnp.exp(scores - log_total)
        d_prob = jnp.dot(dout_block, value_head.T, preferred_element_type=jnp.float32)
        row_delta = lax.optimization_barrier(jnp.sum(weights * d_prob, axis=1, keepdims=True))
        d_score = (weights * (d_prob - row_delta)).astype(jnp.bfloat16)
        grad_query = jnp.dot(d_score, key_rows, preferred_element_type=jnp.float32) * softmax_scale
        grad_key = grad_key + jnp.dot(d_score.T, query_block, preferred_element_type=jnp.float32) * softmax_scale
        grad_value = grad_value + jnp.dot(weights.astype(jnp.bfloat16).T, dout_block, preferred_element_type=jnp.float32)
        return ((grad_key, grad_value), grad_query)
    initial = (jnp.zeros((TOKENS, QK), jnp.float32), jnp.zeros((TOKENS, VD), jnp.float32))
    (grad_key, grad_value), grad_query = lax.scan(visit, initial, jnp.arange(block_count, dtype=jnp.int32))
    return (grad_query.reshape(TOKENS, QK), grad_key, grad_value)

def reference(query, key_nope, key_rope, value, d_out, positions, segments):
    documents = jnp.take(segments, positions).astype(jnp.int32)
    query_heads = query.reshape(TOKENS, HEADS, QK).transpose(1, 0, 2)
    nope_heads = key_nope.reshape(TOKENS, HEADS, NOPE).transpose(1, 0, 2)
    value_heads = value.reshape(TOKENS, HEADS, VD).transpose(1, 0, 2)
    dout_heads = d_out.reshape(TOKENS, HEADS, VD).transpose(1, 0, 2)

    def one_head(operands):
        return head_grads(operands, key_rope, positions, documents)
    grad_query, grad_key, grad_value = lax.map(one_head, (query_heads, nope_heads, value_heads, dout_heads))
    grad_nope = grad_key[:, :, :NOPE]
    grad_rope = lax.optimization_barrier(jnp.sum(grad_key[:, :, NOPE:], axis=0))
    total = jnp.sum(jnp.square(grad_query)) + jnp.sum(jnp.square(grad_nope)) + jnp.sum(jnp.square(grad_rope)) + jnp.sum(jnp.square(grad_value))
    count_all = float(TOKENS * (HEADS * (QK + NOPE + VD) + ROPE))
    factor = jnp.minimum(1.0, 0.25 * math.sqrt(count_all) / jnp.sqrt(total))
    d_query = (grad_query * factor).astype(jnp.bfloat16).transpose(1, 0, 2).reshape(TOKENS, HEADS * QK)
    d_key_nope = (grad_nope * factor).astype(jnp.bfloat16).transpose(1, 0, 2).reshape(TOKENS, HEADS * NOPE)
    d_key_rope = (grad_rope * factor).astype(jnp.bfloat16)
    d_value = (grad_value * factor).astype(jnp.bfloat16).transpose(1, 0, 2).reshape(TOKENS, HEADS * VD)
    return (d_query, d_key_nope, d_key_rope, d_value)
```

```python
import functools
import math

import jax
import jax.numpy as jnp
from jax import lax
from jax.experimental import pallas as pl
from jax.experimental.pallas import tpu as pltpu
from jax.sharding import PartitionSpec as P

NOPE = 128
ROPE = 64
VD = 128
QK = 192
DOCS = 4
CLIP = 0.25
MESH = pl.DeviceIdType.MESH
HIDDEN = -3.0e38
LOWEST = -1.0e30


def grid_of(count):
    width = 1 << (int(math.log2(count)) // 2)
    return count // width, width


def kernel(
    A, B, H, count_all,
    q_in, kn_in, kr_in, v_in, do_in, pos_in, seg_in,
    dq_out, dkn_out, dkr_out, dv_out,
    qb, dob, pqb, knb, krb, vb, pkb,
    stat, statb,
    dqs, dqr, dks, dkr, dvs, dvr, drs, drr,
    n1, n2,
    own_sem, qsend, qrecv, ksend, krecv, ssend, srecv,
    dqsend, dqrecv, dksend, dkrecv, drsend, drrecv, n1send, n1recv, n2send, n2recv,
):
    R = q_in.shape[0]
    NQ, NK = A * R, B * R
    scale = 1.0 / math.sqrt(QK)
    ctx = lax.axis_index("ctx")
    head = lax.axis_index("head")
    a, b = ctx // B, ctx % B

    def a_peer(j):
        return {"ctx": lax.rem(a + j, A) * B + b, "head": head}

    def b_peer(j, g=0):
        return {"ctx": a * B + lax.rem(b + j, B), "head": lax.rem(head + g, H)}

    def remote(src, dst, send, recv, peer):
        return pltpu.make_async_remote_copy(
            src_ref=src, dst_ref=dst, send_sem=send, recv_sem=recv,
            device_id=peer, device_id_type=MESH,
        )

    own = []
    for i, (src, dst) in enumerate((
        (q_in, qb.at[0]), (do_in, dob.at[0]), (pos_in, pqb.at[0]),
        (kn_in, knb.at[0]), (kr_in, krb.at[0]), (v_in, vb.at[0]), (pos_in, pkb.at[0]),
    )):
        copy = pltpu.make_async_copy(src, dst, own_sem.at[i])
        copy.start()
        own.append(copy)

    barrier = pltpu.get_barrier_semaphore()
    peers = [a_peer(j) for j in range(1, A)]
    peers += [b_peer(j, g) for g in range(H) for j in range(B) if (j, g) != (0, 0)]
    for peer in peers:
        pl.semaphore_signal(barrier, inc=1, device_id=peer, device_id_type=MESH)
    pl.semaphore_wait(barrier, len(peers))

    sends = []
    q_copies, k_copies = [], []
    for j in range(1, max(A, B)):
        if j < B:
            for i, (src, buf) in enumerate(((kn_in, knb), (kr_in, krb), (pos_in, pkb), (v_in, vb))):
                k_copies.append(remote(src, buf.at[j], ksend.at[i, j], krecv.at[i, j], b_peer(j)))
                k_copies[-1].start()
        if j < A:
            for i, (src, buf) in enumerate(((q_in, qb), (pos_in, pqb), (do_in, dob))):
                q_copies.append(remote(src, buf.at[j], qsend.at[i, j], qrecv.at[i, j], a_peer(j)))
                q_copies[-1].start()
    sends += q_copies + k_copies

    for copy in own:
        copy.wait()
    for copy in q_copies + k_copies:
        copy.wait_recv()

    q = qb[...].reshape(NQ, QK)
    do = dob[...].reshape(NQ, VD)
    k = jnp.concatenate([knb[...].reshape(NK, NOPE), krb[...].reshape(NK, ROPE)], axis=1)
    v = vb[...].reshape(NK, VD)
    pos_q = jnp.concatenate([pqb[j] for j in range(A)], axis=1)
    seg = seg_in[...]
    start_q = jnp.zeros_like(pos_q)
    for doc in range(1, DOCS):
        first = jnp.sum((seg < doc).astype(jnp.int32))
        start_q = jnp.where(pos_q >= first, first, start_q)
    cols = []
    for j in range(B):
        cols.append(jnp.transpose(jnp.broadcast_to(pkb[j], (R, R))))
    pos_k = jnp.concatenate(cols, axis=0)
    pos_k = jnp.concatenate([pos_k] * A, axis=1)

    nt = (((1,), (1,)), ((), ()))
    s = lax.dot_general(k, q, nt, preferred_element_type=jnp.float32) * scale
    dp = lax.dot_general(v, do, nt, preferred_element_type=jnp.float32)
    vis = (pos_k <= pos_q) & (pos_k >= start_q)
    s = jnp.where(vis, s, HIDDEN)
    m = jnp.maximum(jnp.max(s, axis=0, keepdims=True), LOWEST)
    e = jnp.exp(s - m)
    l = jnp.sum(e, axis=0, keepdims=True)
    wd = jnp.sum(e * dp, axis=0, keepdims=True)

    stat[...] = jnp.concatenate([m, l, wd], axis=1)
    s_copies = []
    for j in range(1, A):
        s_copies.append(remote(stat, statb.at[j], ssend.at[j], srecv.at[j], a_peer(j)))
        s_copies[-1].start()
    sends += s_copies
    ms, ls, wds = [m], [l], [wd]
    for copy in s_copies:
        copy.wait_recv()
    for j in range(1, A):
        got = statb[j]
        parts = []
        for i in range(3):
            one = got[:, i * NQ:(i + 1) * NQ]
            cut = ((A - j) % A) * R
            parts.append(jnp.concatenate([one[:, cut:], one[:, :cut]], axis=1))
        ms.append(parts[0])
        ls.append(parts[1])
        wds.append(parts[2])
    top = functools.reduce(jnp.maximum, ms)
    shrink = [jnp.exp(x - top) for x in ms]
    total_l = sum(x * y for x, y in zip(ls, shrink))
    total_wd = sum(x * y for x, y in zip(wds, shrink))
    inverse = 1.0 / total_l
    f = shrink[0] * inverse
    delta = total_wd * inverse

    w = e * f
    ds = (w * (dp - delta)).astype(jnp.bfloat16)
    wb = w.astype(jnp.bfloat16)
    dk = jnp.dot(ds, q, preferred_element_type=jnp.float32) * scale
    dv = jnp.dot(wb, do, preferred_element_type=jnp.float32)
    dks[...] = dk[:, :NOPE].astype(jnp.bfloat16).reshape(B, R, NOPE)
    drs[...] = dk[:, NOPE:].astype(jnp.bfloat16).reshape(B, R, ROPE)
    dvs[...] = dv.astype(jnp.bfloat16).reshape(B, R, VD)
    g_copies = []
    for j in range(1, B):
        peer = b_peer(B - j)
        g_copies.append(remote(dks.at[j], dkr.at[j], dksend.at[0, j], dkrecv.at[0, j], peer))
        g_copies.append(remote(dvs.at[j], dvr.at[j], dksend.at[1, j], dkrecv.at[1, j], peer))
    rope_slot = b * H + head
    for j in range(B):
        for g in range(H):
            if (j, g) == (0, 0):
                continue
            peer = b_peer(B - j, H - g)
            g_copies.append(
                remote(drs.at[j], drr.at[rope_slot], drsend.at[j, g], drrecv.at[j, g], peer)
            )
    for copy in g_copies:
        copy.start()
    dq = lax.dot_general(ds, k, (((0,), (0,)), ((), ())), preferred_element_type=jnp.float32) * scale
    dqs[...] = dq.astype(jnp.bfloat16).reshape(A, R, QK)
    q_grads = []
    for j in range(1, A):
        q_grads.append(remote(dqs.at[j], dqr.at[j], dqsend.at[j], dqrecv.at[j], a_peer(A - j)))
        q_grads[-1].start()
    drr[rope_slot] = dk[:R, NOPE:].astype(jnp.bfloat16)

    for copy in g_copies[: 2 * (B - 1)]:
        copy.wait_recv()
    gk = dk[:R, :NOPE]
    gv = dv[:R]
    for j in range(1, B):
        gk = gk + dkr[j].astype(jnp.float32)
        gv = gv + dvr[j].astype(jnp.float32)
    for j in range(B):
        for g in range(H):
            if (j, g) == (0, 0):
                continue
            slot = lax.rem(b + j, B) * H + lax.rem(head + g, H)
            remote(drs.at[j], drr.at[slot], drsend.at[j, g], drrecv.at[j, g], b_peer(j, g)).wait_recv()
    gr = drr[0].astype(jnp.float32)
    for i in range(1, B * H):
        gr = gr + drr[i].astype(jnp.float32)
    for copy in q_grads:
        copy.wait_recv()
    gq = dq[:R]
    for j in range(1, A):
        gq = gq + dqr[j].astype(jnp.float32)

    def squares(x):
        return jnp.sum(x * x, axis=0, keepdims=True)

    qs, rs = squares(gq), squares(gr)
    first_head = (head == 0).astype(jnp.float32)
    narrow = qs[:, NOPE:] + rs * first_head
    mine = squares(gk) + squares(gv) + qs[:, :NOPE] + jnp.concatenate(
        [narrow, jnp.zeros_like(narrow)], axis=1)
    n1[rope_slot] = mine
    c1 = []
    for j in range(B):
        for g in range(H):
            if (j, g) == (0, 0):
                continue
            c1.append(remote(n1.at[rope_slot], n1.at[rope_slot], n1send.at[j, g], n1recv.at[j, g],
                             b_peer(B - j, H - g)))
            c1[-1].start()
    for j in range(B):
        for g in range(H):
            if (j, g) == (0, 0):
                continue
            slot = lax.rem(b + j, B) * H + lax.rem(head + g, H)
            remote(n1.at[slot], n1.at[slot], n1send.at[j, g], n1recv.at[j, g], b_peer(j, g)).wait_recv()
    part = n1[0]
    for i in range(1, B * H):
        part = part + n1[i]
    n2[a] = part
    c2 = []
    for j in range(1, A):
        c2.append(remote(n2.at[a], n2.at[a], n2send.at[j], n2recv.at[j], a_peer(A - j)))
        c2[-1].start()
    for j in range(1, A):
        slot = lax.rem(a + j, A)
        remote(n2.at[slot], n2.at[slot], n2send.at[j], n2recv.at[j], a_peer(j)).wait_recv()
    part = n2[0]
    for i in range(1, A):
        part = part + n2[i]
    total = jnp.sum(part, axis=1, keepdims=True)
    factor = jnp.minimum(1.0, CLIP * math.sqrt(count_all) / jnp.sqrt(total))
    dq_out[...] = (gq * factor).astype(jnp.bfloat16)
    dkn_out[...] = (gk * factor).astype(jnp.bfloat16)
    dkr_out[...] = (gr * factor).astype(jnp.bfloat16)
    dv_out[...] = (gv * factor).astype(jnp.bfloat16)
    for copy in sends + g_copies + q_grads + c1 + c2:
        copy.wait_send()


def shards(query, key_nope, key_rope, value, d_out, positions, segments):
    R = query.shape[0]
    n, H = lax.axis_size("ctx"), lax.axis_size("head")
    A, B = grid_of(n)
    NQ = A * R
    count_all = float(R * n * (H * (QK + NOPE + VD) + ROPE))
    bf, f32 = jnp.bfloat16, jnp.float32
    any_spec = pl.BlockSpec(memory_space=pl.ANY)
    vmem = pl.BlockSpec(memory_space=pltpu.VMEM)
    dma = pltpu.SemaphoreType.DMA
    return pl.pallas_call(
        functools.partial(kernel, A, B, H, count_all),
        out_shape=(
            jax.ShapeDtypeStruct((R, QK), bf),
            jax.ShapeDtypeStruct((R, NOPE), bf),
            jax.ShapeDtypeStruct((R, ROPE), bf),
            jax.ShapeDtypeStruct((R, VD), bf),
        ),
        in_specs=[any_spec] * 6 + [vmem],
        out_specs=(vmem,) * 4,
        scratch_shapes=[
            pltpu.VMEM((A, R, QK), bf), pltpu.VMEM((A, R, VD), bf), pltpu.VMEM((A, 1, R), jnp.int32),
            pltpu.VMEM((B, R, NOPE), bf), pltpu.VMEM((B, R, ROPE), bf), pltpu.VMEM((B, R, VD), bf),
            pltpu.VMEM((B, 1, R), jnp.int32),
            pltpu.VMEM((1, 3 * NQ), f32), pltpu.VMEM((A, 1, 3 * NQ), f32),
            pltpu.VMEM((A, R, QK), bf), pltpu.VMEM((A, R, QK), bf),
            pltpu.VMEM((B, R, NOPE), bf), pltpu.VMEM((B, R, NOPE), bf),
            pltpu.VMEM((B, R, VD), bf), pltpu.VMEM((B, R, VD), bf),
            pltpu.VMEM((B, R, ROPE), bf), pltpu.VMEM((B * H, R, ROPE), bf),
            pltpu.VMEM((B * H, 1, 128), f32), pltpu.VMEM((A, 1, 128), f32),
            dma((7,)), dma((3, A)), dma((3, A)), dma((4, B)), dma((4, B)), dma((A,)), dma((A,)),
            dma((A,)), dma((A,)), dma((2, B)), dma((2, B)), dma((B, H)), dma((B, H)),
            dma((B, H)), dma((B, H)), dma((A,)), dma((A,)),
        ],
        compiler_params=pltpu.CompilerParams(
            collective_id=0, has_side_effects=True, vmem_limit_bytes=60 * 1024 * 1024
        ),
        name="mla_backward",
    )(query, key_nope, key_rope, value, d_out, positions.reshape(1, R),
      segments.reshape(-1, 128))


def solution(mesh):
    return jax.shard_map(
        shards,
        mesh=mesh,
        in_specs=(
            P("ctx", "head"),
            P("ctx", "head"),
            P("ctx", None),
            P("ctx", "head"),
            P("ctx", "head"),
            P("ctx"),
            P(),
        ),
        out_specs=(P("ctx", "head"), P("ctx", "head"), P("ctx", None), P("ctx", "head")),
        check_vma=False,
    )
```

```python
import functools
import math

import jax
import jax.numpy as jnp
from jax import lax
from jax.experimental import pallas as pl
from jax.experimental.pallas import tpu as pltpu
from jax.sharding import PartitionSpec as P

NOPE = 128
ROPE = 64
VD = 128
QK = 192
DOCS = 4
CLIP = 0.25
MESH = pl.DeviceIdType.MESH
HIDDEN = -3.0e38
LOWEST = -1.0e30
STAGE = 9


def grid_of(count):
    width = 1 << (int(math.log2(count)) // 2)
    return count // width, width


def flipped(index, mask, size):
    out, bit = 0, 1
    while bit < size:
        digit = lax.rem(index // bit, 2)
        out = out + bit * ((1 - digit) if mask & bit else digit)
        bit *= 2
    return out


def kernel(
    A, B, H,
    qt_in, kn_in, krt_in, v_in, do_in, pos_in, seg_in,
    out_hbm, part_hbm,
    out, segb,
    qb, dob, pqb, knb, krb, vb, pkb,
    stat, statb,
    dqs, dqr, dks, dkr, dvs, dvr, drs, drr,
    norms,
    own_sem, qsend, qrecv, ksend, krecv, ssend, srecv,
    dqsend, dqrecv, dksend, dkrecv, drsend, drrecv, nsend, nrecv, out_sem,
):
    R = kn_in.shape[0]
    NQ, NK = A * R, B * R
    bf, f32 = jnp.bfloat16, jnp.float32
    scale = 1.0 / math.sqrt(QK)
    ctx = lax.axis_index("ctx")
    head = lax.axis_index("head")
    a, b = ctx // B, ctx % B

    def a_peer(j):
        return {"ctx": lax.rem(a + j + A, A) * B + b, "head": head}

    def b_peer(j, g=0):
        return {"ctx": a * B + flipped(b, j, B), "head": lax.rem(head + g, H)}

    def remote(src, dst, send, recv, peer):
        return pltpu.make_async_remote_copy(
            src_ref=src, dst_ref=dst, send_sem=send, recv_sem=recv,
            device_id=peer, device_id_type=MESH,
        )

    others = [(j, g) for g in range(H) for j in range(B) if (j, g) != (0, 0)]
    barrier = pltpu.get_barrier_semaphore()
    peers = [a_peer(j) for j in range(1, A)] + [b_peer(j, g) for j, g in others]
    for peer in peers:
        pl.semaphore_signal(barrier, inc=1, device_id=peer, device_id_type=MESH)

    own = []
    for i, (src, dst) in enumerate((
        (qt_in, qb.at[0]), (do_in, dob.at[0]), (pos_in, pqb.at[0]),
        (kn_in, knb.at[0]), (krt_in, krb.at[0]), (v_in, vb.at[0]), (pos_in, pkb.at[0]),
        (seg_in, segb),
    )):
        copy = pltpu.make_async_copy(src, dst, own_sem.at[i])
        copy.start()
        own.append(copy)
    for copy in own:
        copy.wait()
    pl.semaphore_wait(barrier, len(peers))
    if STAGE == 0:
        return

    sends = []

    def stop():
        for copy in sends:
            copy.wait_send()

    q_copies, k_copies = [], []
    for j in range(1, max(A, B)):
        if j < A:
            for i, buf in enumerate((qb, pqb, dob)):
                q_copies.append(
                    remote(buf.at[0], buf.at[j], qsend.at[i, j], qrecv.at[i, j], a_peer(j)))
                q_copies[-1].start()
        if j < B:
            for i, buf in enumerate((knb, krb, pkb, vb)):
                k_copies.append(
                    remote(buf.at[0], buf.at[j], ksend.at[i, j], krecv.at[i, j], b_peer(j)))
                k_copies[-1].start()
    sends += q_copies + k_copies

    seg = segb[...]
    firsts = [jnp.sum((seg < doc).astype(jnp.int32)) for doc in range(1, DOCS)]
    for copy in q_copies + k_copies:
        copy.wait_recv()
    if STAGE == 1:
        return stop()

    qt = jnp.concatenate([qb[j] for j in range(A)], axis=1)
    do = dob[...].reshape(NQ, VD)
    kr = jnp.concatenate([jnp.transpose(krb[j]) for j in range(B)], axis=0)
    k = jnp.concatenate([knb[...].reshape(NK, NOPE), kr], axis=1)
    v = vb[...].reshape(NK, VD)
    pos_q = jnp.concatenate([pqb[j] for j in range(A)], axis=1)
    start_q = jnp.zeros_like(pos_q)
    for first in firsts:
        start_q = jnp.where(pos_q >= first, first, start_q)
    pos_k = jnp.concatenate(
        [jnp.transpose(jnp.broadcast_to(pkb[j], (R, R))) for j in range(B)], axis=0)
    pos_k = jnp.concatenate([pos_k] * A, axis=1)

    nt = (((1,), (1,)), ((), ()))
    s = jnp.dot(k, qt, preferred_element_type=f32) * scale
    dp = lax.dot_general(v, do, nt, preferred_element_type=f32)
    vis = (pos_k <= pos_q) & (pos_k >= start_q)
    s = jnp.where(vis, s, HIDDEN)
    m = jnp.maximum(jnp.max(s, axis=0, keepdims=True), LOWEST)
    e = jnp.exp(s - m)
    l = jnp.sum(e, axis=0, keepdims=True)
    wd = jnp.sum(e * dp, axis=0, keepdims=True)

    stat[...] = jnp.concatenate([m, l, wd], axis=1)
    if STAGE == 2:
        return stop()
    s_copies = []
    for j in range(1, A):
        s_copies.append(remote(stat, statb.at[j], ssend.at[j], srecv.at[j], a_peer(j)))
        s_copies[-1].start()
    sends += s_copies
    ms, ls, wds = [m], [l], [wd]
    for copy in s_copies:
        copy.wait_recv()
    if STAGE == 3:
        return stop()
    for j in range(1, A):
        got = statb[j]
        parts = []
        for i in range(3):
            one = got[:, i * NQ:(i + 1) * NQ]
            cut = ((A - j) % A) * R
            parts.append(jnp.concatenate([one[:, cut:], one[:, :cut]], axis=1))
        ms.append(parts[0])
        ls.append(parts[1])
        wds.append(parts[2])
    top = functools.reduce(jnp.maximum, ms)
    shrink = [jnp.exp(x - top) for x in ms]
    total_l = sum(x * y for x, y in zip(ls, shrink))
    total_wd = sum(x * y for x, y in zip(wds, shrink))
    inverse = 1.0 / total_l
    f = shrink[0] * inverse
    delta = total_wd * inverse

    w = e * f
    ds = (w * (dp - delta)).astype(bf)
    kt = jnp.concatenate(
        [jnp.concatenate([jnp.transpose(knb[j]) for j in range(B)], axis=1),
         jnp.concatenate([krb[j] for j in range(B)], axis=1)], axis=0)
    dqt = jnp.dot(kt, ds, preferred_element_type=f32) * scale
    q_grads = []
    for j in range(1, A):
        dqs[j] = dqt[:, j * R:(j + 1) * R].astype(bf)
        q_grads.append(remote(dqs.at[j], dqr.at[j], dqsend.at[j], dqrecv.at[j], a_peer(-j)))
        q_grads[-1].start()
    g_copies = []
    rope_slot = b * H + head
    dv = jnp.dot(w.astype(bf), do, preferred_element_type=f32)
    dvs[...] = dv.astype(bf).reshape(B, R, VD)
    for j in range(1, B):
        g_copies.append(remote(dvs.at[j], dvr.at[j], dksend.at[1, j], dkrecv.at[1, j], b_peer(j)))
        g_copies[-1].start()
    dk = lax.dot_general(ds, qt, nt, preferred_element_type=f32) * scale
    drt = []
    for j in range(B):
        drt.append(jnp.transpose(dk[j * R:(j + 1) * R, NOPE:]).astype(bf))
        drs[j] = drt[j]
    dks[...] = dk[:, :NOPE].astype(bf).reshape(B, R, NOPE)
    for j, g in others:
        g_copies.append(remote(
            drs.at[j], drr.at[rope_slot], drsend.at[j, g], drrecv.at[j, g], b_peer(j, H - g)))
    for j in range(1, B):
        g_copies.append(remote(dks.at[j], dkr.at[j], dksend.at[0, j], dkrecv.at[0, j], b_peer(j)))
    for copy in g_copies[B - 1:]:
        copy.start()
    sends += g_copies + q_grads
    drr[rope_slot] = drt[0]

    for copy in g_copies[: B - 1] + g_copies[len(g_copies) - B + 1:]:
        copy.wait_recv()
    gk = dk[:R, :NOPE]
    gv = dv[:R]
    for j in range(1, B):
        gk = gk + dkr[j].astype(f32)
        gv = gv + dvr[j].astype(f32)
    for j, g in others:
        slot = flipped(b, j, B) * H + lax.rem(head + g, H)
        remote(drs.at[j], drr.at[slot], drsend.at[j, g], drrecv.at[j, g], b_peer(j, g)).wait_recv()
    gr = drr[0].astype(f32)
    for i in range(1, B * H):
        gr = gr + drr[i].astype(f32)
    for copy in q_grads:
        copy.wait_recv()
    gq = dqt[:, :R]
    for j in range(1, A):
        gq = gq + dqr[j].astype(f32)

    def squares(x):
        return jnp.sum(x * x, axis=0, keepdims=True)

    first_head = (head == 0).astype(f32)
    mine = squares(gk) + squares(gv) + squares(gq) + squares(gr) * first_head
    place = ctx * H + head
    norms[place] = mine
    everyone = [(i, j, g) for g in range(H) for i in range(A) for j in range(B) if (i, j, g) != (0, 0, 0)]

    def norm_copy(i, j, g, slot, way):
        peer = {"ctx": lax.rem(a + way * i + A, A) * B + flipped(b, j, B),
                "head": lax.rem(head + way * g + H, H)}
        slot = peer["ctx"] * H + peer["head"] if slot is None else slot
        return remote(norms.at[slot], norms.at[slot], nsend.at[i, j, g], nrecv.at[i, j, g], peer)

    if STAGE != 5:
        for i, j, g in everyone:
            sends.append(norm_copy(i, j, g, place, 1))
            sends[-1].start()
    top_q, top_k, top_r = QK, QK + R, QK + R + ROPE
    out[:top_q, :] = gq
    out[top_q:top_k, :] = gk
    out[top_k:top_r, :] = gr
    out[top_r:, :] = gv
    put = pltpu.make_async_copy(out, out_hbm, out_sem.at[0])
    put.start()
    if STAGE != 5:
        for i, j, g in everyone:
            norm_copy(i, j, g, None, -1).wait_recv()
    part = pltpu.make_async_copy(norms, part_hbm, out_sem.at[1])
    part.start()
    put.wait()
    part.wait()
    stop()


def finish(count_all, grads, part, dq_out, dkn_out, dkr_out, dv_out):
    total = jnp.sum(jnp.sum(part[...], axis=0), axis=1, keepdims=True)
    factor = jnp.minimum(1.0, CLIP * math.sqrt(count_all) / jnp.sqrt(total))
    row = 0
    for dst in (dq_out, dkn_out, dkr_out, dv_out):
        rows = dst.shape[0]
        dst[...] = (grads[row:row + rows, :] * factor).astype(dst.dtype)
        row += rows


def shards(query, key_nope, key_rope, value, d_out, positions, segments):
    R = query.shape[0]
    n, H = lax.axis_size("ctx"), lax.axis_size("head")
    A, B = grid_of(n)
    NQ = A * R
    count_all = float(R * n * (H * (QK + NOPE + VD) + ROPE))
    bf, f32 = jnp.bfloat16, jnp.float32
    any_spec = pl.BlockSpec(memory_space=pl.ANY)
    vmem = pl.BlockSpec(memory_space=pltpu.VMEM)
    dma = pltpu.SemaphoreType.DMA
    rows = QK + R + ROPE + R
    grads, part = pl.pallas_call(
        functools.partial(kernel, A, B, H),
        out_shape=(
            jax.ShapeDtypeStruct((rows, R), f32),
            jax.ShapeDtypeStruct((n * H, 1, 128), f32),
        ),
        in_specs=[any_spec] * 7,
        out_specs=(any_spec, any_spec),
        scratch_shapes=[
            pltpu.VMEM((rows, R), f32), pltpu.VMEM((n * R // 128, 128), jnp.int32),
            pltpu.VMEM((A, QK, R), bf), pltpu.VMEM((A, R, VD), bf), pltpu.VMEM((A, 1, R), jnp.int32),
            pltpu.VMEM((B, R, NOPE), bf), pltpu.VMEM((B, ROPE, R), bf), pltpu.VMEM((B, R, VD), bf),
            pltpu.VMEM((B, 1, R), jnp.int32),
            pltpu.VMEM((1, 3 * NQ), f32), pltpu.VMEM((A, 1, 3 * NQ), f32),
            pltpu.VMEM((A, QK, R), bf), pltpu.VMEM((A, QK, R), bf),
            pltpu.VMEM((B, R, NOPE), bf), pltpu.VMEM((B, R, NOPE), bf),
            pltpu.VMEM((B, R, VD), bf), pltpu.VMEM((B, R, VD), bf),
            pltpu.VMEM((B, ROPE, R), bf), pltpu.VMEM((B * H, ROPE, R), bf),
            pltpu.VMEM((n * H, 1, 128), f32),
            dma((8,)), dma((3, A)), dma((3, A)), dma((4, B)), dma((4, B)), dma((A,)), dma((A,)),
            dma((A,)), dma((A,)), dma((2, B)), dma((2, B)), dma((B, H)), dma((B, H)),
            dma((A, B, H)), dma((A, B, H)), dma((2,)),
        ],
        compiler_params=pltpu.CompilerParams(
            collective_id=0, has_side_effects=True, vmem_limit_bytes=60 * 1024 * 1024
        ),
        name="mla_backward",
    )(query.T, key_nope, key_rope.T, value, d_out, positions.reshape(1, R),
      segments.reshape(-1, 128))
    dqt, dkn, dkrt, dv = pl.pallas_call(
        functools.partial(finish, count_all),
        out_shape=(
            jax.ShapeDtypeStruct((QK, R), bf),
            jax.ShapeDtypeStruct((R, NOPE), bf),
            jax.ShapeDtypeStruct((ROPE, R), bf),
            jax.ShapeDtypeStruct((R, VD), bf),
        ),
        in_specs=[vmem, vmem],
        out_specs=(vmem,) * 4,
        name="clip",
    )(grads, part)
    return dqt.T, dkn, dkrt.T, dv


def solution(mesh):
    return jax.shard_map(
        shards,
        mesh=mesh,
        in_specs=(
            P("ctx", "head"),
            P("ctx", "head"),
            P("ctx", None),
            P("ctx", "head"),
            P("ctx", "head"),
            P("ctx"),
            P(),
        ),
        out_specs=(P("ctx", "head"), P("ctx", "head"), P("ctx", None), P("ctx", "head")),
        check_vma=False,
    )
```
